32 devices in a mesh: segment: 4 (over z), row: 4 (over y, x), col: 2 (over core).
Axes of the slice: x: 2, y: 2, z: 4, core: 2. Of those that a mesh axis runs over, the one named last changes fastest.
Arguments:
- frames: bfloat16 [2, 64, 32, 128], P(None, 'row', 'col'), may hold values from -6 to 6
- caches: bfloat16 [4, 2, 2, 64, 32, 128], P('segment', None, None, 'row', 'col'), may hold values from -5 to 5
- weights: bfloat16 [4, 2, 3, 3, 3, 128, 128], P('segment'), may hold values from -0.109375 to 0.109375
- biases: float32 [4, 2, 128], P('segment'), may hold values from -0.5 to 0.5
- gains: float32 [4, 2, 128], P('segment'), may hold values from 0.1 to 1.9
Outputs:
- sections: bfloat16 [4, 2, 64, 32, 128], P('segment', None, 'row', 'col')
The draws below stay inside these ranges and needn't reach their ends.
All inputs are finite; a program needn't handle non-finite values.
Results may differ from the reference program's by a relative error of at most 0.0055.
Values may be sent and summed in bfloat16 or wider, within the bound.
A program may use at most 64 MiB of HBM per device.

```python
import jax
import jax.numpy as jnp
from jax import lax

C = 128
SECTIONS = 4
FRAMES = 2
H = 64
W = 32
N_SEGMENT = 4


def shard_levels(key, shape, pieces, smallest, high):
    loudness, own = 1.0, jax.random.fold_in(key, 6)
    for position, shards_of in pieces:
        draws = jnp.exp(jax.random.uniform(jax.random.fold_in(own, position), (shards_of,), jnp.float32, smallest / len(pieces), high / len(pieces)))
        loudness = loudness * jnp.repeat(draws, shape[position] // shards_of).reshape([-1 if axis == position else 1 for axis in range(len(shape))])
    return loudness


def centred(own_key, extent, spread, limit, shards=(), dtype=jnp.bfloat16):
    entries = jax.random.normal(own_key, extent, jnp.float32) * spread
    if len(shards) > 0:
        entries = shard_levels(own_key, extent, shards, -0.22, 0.18) * entries
    return jnp.clip(entries, min=-limit, max=limit).astype(dtype)


def setup_inputs(seed: int = 0) -> dict:
    streams_of = jax.random.split(jax.random.key(seed), 6)
    return {
        "frames": centred(streams_of[0], (FRAMES, H, W, C), 1.0, 6.0, ((1, 4), (2, 2))),
        "caches": centred(streams_of[1], (SECTIONS, 2, 2, H, W, C), 0.7, 5.0, ((0, 4), (3, 4), (4, 2))),
        "weights": centred(streams_of[2], (SECTIONS, 2, 3, 3, 3, C, C), (27 * C) ** -0.5, 0.109375, ((0, 4),)),
        "biases": jnp.clip(jax.random.uniform(streams_of[3], (SECTIONS, 2, C), jnp.float32, -0.5, 0.5) * shard_levels(streams_of[3], (SECTIONS, 2, C), ((0, 4),), -0.4, 0.0), -0.5, 0.5),
        "gains": jnp.clip(1.0 + 0.18 * jax.random.normal(streams_of[4], (SECTIONS, 2, C), jnp.float32), 0.1, 1.9),
    }


def norm_act(values, gain_row):
    values = values.astype(jnp.float32)
    scaled = values * jax.lax.rsqrt(lax.optimization_barrier(jnp.mean(values * values, axis=-1, keepdims=True)) + 1e-06) * gain_row
    return jax.nn.silu(scaled).astype(jnp.bfloat16)

def convolve(sequence, previous, kernel, bias_row):
    joined = jnp.concatenate([previous, sequence], axis=0)
    padded = jnp.pad(joined, ((0, 0), (1, 1), (1, 1), (0, 0)))
    frame_count = sequence.shape[0]
    rows = sequence.shape[1]
    cols = sequence.shape[2]
    accum = jnp.zeros(sequence.shape[:3] + (kernel.shape[-1],), jnp.float32)
    for tap_t in range(3):
        for tap_h in range(3):
            for tap_w in range(3):
                slab = padded[tap_t:tap_t + frame_count, tap_h:tap_h + rows, tap_w:tap_w + cols].astype(jnp.float32)
                accum = accum + jnp.einsum('fhwc,co->fhwo', slab, kernel[tap_t, tap_h, tap_w].astype(jnp.float32))
    return accum + bias_row

def reference(frames, caches, weights, biases, gains):
    current = frames
    results = []
    for section in range(N_SEGMENT):
        normed_one = norm_act(current, gains[section, 0])
        hidden = convolve(normed_one, caches[section, 0], weights[section, 0], biases[section, 0])
        normed_two = norm_act(hidden, gains[section, 1])
        branch = convolve(normed_two, caches[section, 1], weights[section, 1], biases[section, 1])
        current = (current.astype(jnp.float32) + branch).astype(jnp.bfloat16)
        results.append(current)
    return jnp.stack(results, axis=0)
```

```python
import functools

import jax
import jax.numpy as jnp
from jax import lax
from jax.experimental import pallas as pl
from jax.experimental.pallas import tpu as pltpu
from jax.sharding import PartitionSpec as P

EDGE = 8
STRIP = 2
TAPS = 3
AROUND = [(dr, dc) for dr in (-1, 1, 0) for dc in (0, -1, 1) if (dr, dc) != (0, 0)]
MID, OUTER = 0, 1


def neighbours(count):
    return {1: (0,), 2: (1,)}.get(count, (1, 2))


def norm_act(values, gain_row):
    scale = lax.rsqrt(jnp.mean(values * values, axis=-1, keepdims=True) + 1e-06)
    half = 0.5 * (values * scale * gain_row)
    return half * jnp.tanh(half) + half


def shifted(values):
    size = values.shape[0]
    return pltpu.roll(values, 1, 0), values, pltpu.roll(values, size - 1, 0)


def kernel(
    counts,
    frames, caches, weights_in, biases_in, gains_in,
    out,
    weights, biases, gains, x_pad, one_pad, two_pad, taps_one, taps_two,
    held_taps_one, held_taps_two, sum_one, sum_two, inside,
    send_sem, recv_sem, local_sem, ready_sem,
):
    segments, tile_rows_n, tile_cols_n = counts
    seg, row, col = (lax.axis_index(name) for name in ("segment", "row", "col"))
    total, rows, cols, channels = frames.shape
    pitch = cols + EDGE
    first = seg == 0
    later = seg > 0
    more = seg < segments - 1

    def exists(dr, dc):
        r, c = row + dr, col + dc
        return (r >= 0) & (r < tile_rows_n) & (c >= 0) & (c < tile_cols_n)

    def device(dz, dr, dc):
        return {"segment": seg + dz, "row": row + dr, "col": col + dc}

    def number(flag):
        return flag.astype(jnp.int32)

    ups = number(row > 0) + number(row < tile_rows_n - 1)
    sides = number(col > 0) + number(col < tile_cols_n - 1)

    def local(source, target, which):
        return pltpu.make_async_copy(source, target, local_sem.at[which])

    def source_rows(dr, base, halo):
        if dr == 0:
            return pl.ds(base, rows)
        return pl.ds(base if dr < 0 else base + rows - halo, halo)

    def source_cols(dc, base):
        if dc == 0:
            return pl.ds(base, cols)
        return pl.ds(base if dc < 0 else base + cols - STRIP, STRIP)

    def target_rows(dr, dc, halo):
        skip = 1 if dc < 0 else 0
        if dr == 0:
            return pl.ds(halo + skip, rows)
        return pl.ds((halo + rows if dr < 0 else 0) + skip, halo)

    def target_cols(dc):
        if dc == 0:
            return pl.ds(EDGE, cols)
        return pl.ds(0, STRIP) if dc < 0 else pl.ds(EDGE - STRIP, STRIP)

    def remote(source, target, halo, send, recv, dz, dr, dc):
        top, left = (0, 0) if dz else (halo, EDGE)
        lead = (slice(None),) * (len(source.shape) - 3)
        group = OUTER if dr else MID
        return pltpu.make_async_remote_copy(
            src_ref=source.at[lead + (source_rows(dr, top, halo), source_cols(dc, left))],
            dst_ref=target.at[lead + (target_rows(dr, dc, halo), target_cols(dc))],
            send_sem=send_sem.at[send, group],
            recv_sem=recv_sem.at[recv, group],
            device_id=device(dz, dr, dc),
            device_id_type=pl.DeviceIdType.MESH,
        )

    held = [(one_pad, one_pad, 2, 0, 0, 0), (two_pad, two_pad, 1, 1, 1, 0)]
    begin = [(x_pad.at[f], x_pad.at[f], 2, 2 + f, 2 + f, 0) for f in range(total)]
    onward = [(out.at[f], x_pad.at[f], 2, 2 + total + f, 2 + f, 1) for f in range(total)]

    def start(stream, allowed, outer):
        for dr, dc in AROUND:
            if dr not in outer:
                continue
            good = exists(dr, dc)
            if allowed is not None:
                good = good & allowed

            @pl.when(good)
            def _():
                remote(*stream, dr, dc).start()

    def settle(sem, view, options, allowed):
        for up in options[0]:
            for side in options[1]:
                shape = view(up, side)
                if shape is None:
                    continue
                good = (ups == up) & (sides == side)
                if allowed is not None:
                    good = good & allowed

                @pl.when(good)
                def _():
                    pltpu.make_async_copy(shape, shape, sem).wait()

    up_options, side_options = neighbours(tile_rows_n), neighbours(tile_cols_n)

    def cut(ref, height, width):
        if height == 0 or width == 0:
            return None
        lead = (slice(None),) * (len(ref.shape) - 3)
        return ref.at[lead + (pl.ds(0, height), pl.ds(0, width))]

    def settle_group(sems, which, stream, group, allowed, centre):
        ref, halo = stream[1], stream[2]
        middle = cols if centre else 0
        if group == MID:
            view = lambda up, side: cut(ref, rows, middle + STRIP * side)
        else:
            view = lambda up, side: cut(ref, halo * up, cols + STRIP * side)
        settle(sems.at[which, group], view, (up_options, side_options), allowed)

    def received(stream, group, allowed=None, centre=False):
        settle_group(recv_sem, stream[4], stream, group, allowed, centre)

    def sent(stream, allowed=None, centre=False):
        for group in (MID, OUTER):
            settle_group(send_sem, stream[3], stream, group, allowed, centre)

    edge = rows // 4 if rows % 4 == 0 else rows // 2
    pieces = [(0, edge), (rows - edge, edge)] + ([(edge, rows - 2 * edge)] if rows > 2 * edge else [])

    def tile_copy(f, low, size):
        return pltpu.make_async_remote_copy(
            src_ref=out.at[f, pl.ds(low, size)],
            dst_ref=x_pad.at[f, pl.ds(2 + low, size), pl.ds(EDGE, cols)],
            send_sem=send_sem.at[2 + total + f, MID],
            recv_sem=recv_sem.at[2 + f, MID],
            device_id=device(1, 0, 0),
            device_id_type=pl.DeviceIdType.MESH,
        )

    centre_of = lambda pad, halo: pad.at[:, pl.ds(halo, rows), pl.ds(EDGE, cols)]
    own = local(frames, centre_of(x_pad, 2), 0)
    held_copies = [local(caches.at[0], centre_of(one_pad, 2), 1), local(caches.at[1], centre_of(two_pad, 1), 2)]
    parameters = [
        local(biases_in, biases, 3),
        local(gains_in, gains, 4),
        local(weights_in.at[0], weights.at[0], 5),
        local(weights_in.at[1], weights.at[1], 6),
    ]

    @pl.when(first)
    def _():
        own.start()

    for copy in held_copies + parameters:
        copy.start()

    for pad, halo in ((x_pad, 2), (one_pad, 2), (two_pad, 1)):
        count, height = pad.shape[0], pad.shape[1]
        pad[:, :, 0:EDGE] = jnp.zeros((count, height, EDGE, channels), pad.dtype)
        pad[:, 0:halo, EDGE:] = jnp.zeros((count, halo, cols, channels), pad.dtype)
        pad[:, halo + rows :, EDGE:] = jnp.zeros((count, height - halo - rows, cols, channels), pad.dtype)

    def signal_all(semaphore, steps):
        for dz in steps:
            for dr, dc in AROUND + [(0, 0)]:
                if (dz, dr, dc) == (0, 0, 0):
                    continue

                @pl.when(exists(dr, dc) & (seg + dz >= 0) & (seg + dz < segments))
                def _():
                    pl.semaphore_signal(
                        semaphore, inc=1, device_id=device(dz, dr, dc),
                        device_id_type=pl.DeviceIdType.MESH,
                    )

    plane = (ups + 1) * (sides + 1)
    barrier = pltpu.get_barrier_semaphore()
    signal_all(barrier, (0, 1))
    pl.semaphore_wait(barrier, plane - 1 + plane * number(later))

    @pl.when(first)
    def _():
        own.wait()

    start(begin[0], first, (-1, 1, 0))
    held_copies[0].wait()
    start(held[0], None, (-1, 1, 0))
    held_copies[1].wait()
    start(held[1], None, (-1, 1, 0))
    for f in range(1, total):
        start(begin[f], first, (-1, 1, 0))
    signal_all(ready_sem, (-1,))

    cell = lax.broadcasted_iota(jnp.int32, inside.shape, 0)
    place = cell % pitch
    wrapped = place < EDGE // 2
    cell_row = row * rows + cell // pitch - 1 - number(wrapped)
    cell_col = col * cols + place - EDGE + jnp.where(wrapped, EDGE + cols, 0)
    inside[...] = jnp.where(
        (cell_row >= 0) & (cell_row < rows * tile_rows_n)
        & (cell_col >= 0) & (cell_col < cols * tile_cols_n), 1.0, 0.0,
    )

    def kernel_of(which, *times):
        return jnp.concatenate([weights[which, t] for t in times], axis=1)

    def patches(store, step, parts):
        return jnp.concatenate(
            [
                jnp.concatenate([store[pl.ds(low + dh * step, size), :] for low, size in parts], axis=0)
                for dh in range(TAPS)
            ],
            axis=1,
        )

    def product(store, step, parts, matrix):
        return jnp.dot(patches(store, step, parts), matrix, preferred_element_type=jnp.float32)

    def flat(pad, index, low, high):
        values = pad[index, low:high].astype(jnp.float32)
        return values.reshape((high - low) * pitch, channels)

    def put_all(store, low, values, skip, size):
        for tap, part in enumerate(shifted(values)):
            store[pl.ds(low, size), tap * channels : (tap + 1) * channels] = (
                part[skip : skip + size].astype(jnp.bfloat16)
            )

    def put_tile(store, low, values, height):
        for tap, part in enumerate(shifted(values)):
            part = part[: height * pitch].reshape(height, pitch, channels)[:, EDGE:]
            store[pl.ds(low * cols, height * cols), tap * channels : (tap + 1) * channels] = (
                part.reshape(height * cols, channels).astype(jnp.bfloat16)
            )

    def add_cached(which, store, sums, step, parts):
        bias = biases[which : which + 1]
        older = product(store.at[0], step, parts, kernel_of(which, 0))
        newer = product(store.at[1], step, parts, kernel_of(which, 1, 0))
        at = 0
        for low, size in parts:
            here = slice(at, at + size)
            sums[0, pl.ds(low, size)] = older[here] + newer[here, :channels] + bias
            sums[1, pl.ds(low, size)] = newer[here, channels:] + bias
            at += size

    for copy in parameters:
        copy.wait()

    whole = sum_one.shape[1]
    brim = -(-(3 * pitch + EDGE) // 16) * 16
    rest = (rows - 1) * pitch // 16 * 16
    received(held[0], MID)
    for frame in range(2):
        put_all(
            held_taps_one.at[frame], 3 * pitch, flat(one_pad, frame, 3, rows + 2), 0, (rows - 1) * pitch
        )
    low = 3 * pitch
    add_cached(0, held_taps_one, sum_one, pitch, [(low, (rows - 1) * pitch + EDGE - low)])
    received(held[1], MID)
    for frame in range(2):
        put_tile(held_taps_two.at[frame], 2, flat(two_pad, frame, 2, rows + 1), rows - 2)
    add_cached(1, held_taps_two, sum_two, cols, [(2 * cols, (rows - 4) * cols)])

    received(held[0], OUTER)
    for frame in range(2):
        put_all(held_taps_one.at[frame], 0, flat(one_pad, frame, 0, 5), 0, brim)
        values = flat(one_pad, frame, rows, rows + 5)
        put_all(held_taps_one.at[frame], rows * pitch + EDGE, values, EDGE, 5 * pitch - EDGE)
    add_cached(0, held_taps_one, sum_one, pitch, [(0, brim), (rest, whole - rest)])
    received(held[1], OUTER)
    for frame in range(2):
        put_tile(held_taps_two.at[frame], 0, flat(two_pad, frame, 0, 3), 2)
        put_tile(held_taps_two.at[frame], rows, flat(two_pad, frame, rows, rows + 3), 2)
    add_cached(1, held_taps_two, sum_two, cols, [(0, 2 * cols), ((rows - 2) * cols, 2 * cols)])

    @pl.when(more)
    def _():
        pl.semaphore_wait(ready_sem, plane)

    half = (rows + 2) // 4 * 2
    blocks = [(0, half), (half, rows + 2 - half)]

    for f in range(total):
        for group in (MID, OUTER):
            received(begin[f], group, first)
            received(onward[f], group, later, group == MID)

        values = norm_act(flat(x_pad, f, 0, rows + 5), gains[0:1])
        put_all(taps_one, 0, values, 0, (rows + 5) * pitch)
        times = (2, 1) if f == 0 else (2,)
        for low, height in blocks:
            last = low + height == rows + 2
            size = whole - low * pitch if last else height * pitch + EDGE
            part = pl.ds(low * pitch, size)
            fresh = product(taps_one, pitch, [(low * pitch, size)], kernel_of(0, *times))
            hidden = sum_one[f, part] + fresh[:, :channels]
            if f == 0:
                keep = size if last else height * pitch
                sum_one[1, pl.ds(low * pitch, keep)] += fresh[:keep, channels:]
            put_tile(taps_two, low, norm_act(hidden, gains[1:2]) * inside[part], height)
        for group in (pieces[:2], pieces[2:]):
            if not group:
                continue
            parts = [(low * cols, size * cols) for low, size in group]
            fresh = product(taps_two, cols, parts, kernel_of(1, *times))
            at = 0
            for low, size in group:
                here = slice(at, at + size * cols)
                part = pl.ds(low * cols, size * cols)
                branch = sum_two[f, part] + fresh[here, :channels]
                if f == 0:
                    sum_two[1, part] += fresh[here, channels:]
                inputs = x_pad[f, 2 + low : 2 + low + size, EDGE:].astype(jnp.float32)
                out[f, low : low + size] = (inputs + branch.reshape(size, cols, channels)).astype(out.dtype)
                at += size * cols
            if group[0][0] == 0:
                start(onward[f], more, (-1, 1))
            if group[-1] is pieces[-1]:
                start(onward[f], more, (0,))

            @pl.when(more)
            def _():
                for low, size in group:
                    tile_copy(f, low, size).start()

    for stream in held:
        sent(stream)
    for f in range(total):
        sent(begin[f], first)
        sent(onward[f], more, True)


def solution(mesh):
    counts = tuple(mesh.shape[name] for name in ("segment", "row", "col"))

    def on_device(frames, caches, weights, biases, gains):
        total, rows, cols, channels = frames.shape
        pitch = cols + EDGE
        whole = -(-((rows + 2) * pitch + EDGE) // 16) * 16
        bf16, f32 = jnp.bfloat16, jnp.float32
        vmem = pl.BlockSpec(memory_space=pltpu.VMEM)
        taps = weights.reshape(2, TAPS, TAPS * TAPS * channels, channels)
        result = pl.pallas_call(
            functools.partial(kernel, counts),
            out_shape=pltpu.VMEM(frames.shape, bf16),
            in_specs=[pl.BlockSpec(memory_space=pl.ANY)] * 5,
            out_specs=vmem,
            scratch_shapes=[
                pltpu.VMEM(taps.shape, bf16),
                pltpu.VMEM(biases.shape[1:], f32),
                pltpu.VMEM(gains.shape[1:], f32),
                pltpu.VMEM((total, rows + 5, pitch, channels), bf16),
                pltpu.VMEM((2, rows + 5, pitch, channels), bf16),
                pltpu.VMEM((2, rows + 3, pitch, channels), bf16),
                pltpu.VMEM(((rows + 5) * pitch, TAPS * channels), bf16),
                pltpu.VMEM(((rows + 2) * cols, TAPS * channels), bf16),
                pltpu.VMEM((2, (rows + 5) * pitch, TAPS * channels), bf16),
                pltpu.VMEM((2, (rows + 2) * cols, TAPS * channels), bf16),
                pltpu.VMEM((total, whole, channels), f32),
                pltpu.VMEM((total, rows * cols, channels), f32),
                pltpu.VMEM((whole, channels), f32),
                pltpu.SemaphoreType.DMA((2 + 2 * total, 2)),
                pltpu.SemaphoreType.DMA((2 + total, 2)),
                pltpu.SemaphoreType.DMA((7,)),
                pltpu.SemaphoreType.REGULAR,
            ],
            compiler_params=pltpu.CompilerParams(collective_id=0, has_side_effects=True),
        )(frames, caches[0], taps, biases[0], gains[0])
        return result[None]

    in_specs = (
        P(None, "row", "col", None),
        P("segment", None, None, "row", "col", None),
        P("segment", None, None, None, None, None, None),
        P("segment", None, None),
        P("segment", None, None),
    )
    out_specs = P("segment", None, "row", "col", None)
    return jax.shard_map(
        on_device, mesh=mesh, in_specs=in_specs, out_specs=out_specs, check_vma=False
    )
```

```python
import functools

import jax
import jax.numpy as jnp
from jax import lax
from jax.experimental import pallas as pl
from jax.experimental.pallas import tpu as pltpu
from jax.sharding import PartitionSpec as P

EDGE = 8
STRIP = 2
TAPS = 3
AROUND = [(dr, dc) for dr in (-1, 1, 0) for dc in (0, -1, 1) if (dr, dc) != (0, 0)]
MID, OUTER = 0, 1


def neighbours(count):
    return {1: (0,), 2: (1,)}.get(count, (1, 2))


def norm_act(values, gain_row):
    scale = lax.rsqrt(jnp.mean(values * values, axis=-1, keepdims=True) + 1e-06)
    half = 0.5 * (values * scale * gain_row)
    return half * jnp.tanh(half) + half


def shifted(values):
    size = values.shape[0]
    return pltpu.roll(values, 1, 0), values, pltpu.roll(values, size - 1, 0)


def kernel(
    counts,
    frames, caches, weights_in, biases_in, gains_in,
    out,
    weights, biases, gains, x_pad, one_pad, two_pad, taps_one, taps_two,
    held_taps_one, held_taps_two, sum_one, sum_two, inside,
    send_sem, recv_sem, local_sem, ready_sem,
):
    segments, tile_rows_n, tile_cols_n = counts
    seg, row, col = (lax.axis_index(name) for name in ("segment", "row", "col"))
    total, rows, cols, channels = frames.shape
    pitch = cols + EDGE
    first = seg == 0
    later = seg > 0
    more = seg < segments - 1

    def exists(dr, dc):
        r, c = row + dr, col + dc
        return (r >= 0) & (r < tile_rows_n) & (c >= 0) & (c < tile_cols_n)

    def device(dz, dr, dc):
        return {"segment": seg + dz, "row": row + dr, "col": col + dc}

    def number(flag):
        return flag.astype(jnp.int32)

    ups = number(row > 0) + number(row < tile_rows_n - 1)
    sides = number(col > 0) + number(col < tile_cols_n - 1)

    def local(source, target, which):
        return pltpu.make_async_copy(source, target, local_sem.at[which])

    def source_rows(dr, base, halo):
        if dr == 0:
            return pl.ds(base, rows)
        return pl.ds(base if dr < 0 else base + rows - halo, halo)

    def source_cols(dc, base):
        if dc == 0:
            return pl.ds(base, cols)
        return pl.ds(base if dc < 0 else base + cols - STRIP, STRIP)

    def target_rows(dr, dc, halo):
        skip = 1 if dc < 0 else 0
        if dr == 0:
            return pl.ds(halo + skip, rows)
        return pl.ds((halo + rows if dr < 0 else 0) + skip, halo)

    def target_cols(dc):
        if dc == 0:
            return pl.ds(EDGE, cols)
        return pl.ds(0, STRIP) if dc < 0 else pl.ds(EDGE - STRIP, STRIP)

    def remote(source, target, halo, send, recv, dz, dr, dc):
        top, left = (0, 0) if dz else (halo, EDGE)
        lead = (slice(None),) * (len(source.shape) - 3)
        group = OUTER if dr else MID
        return pltpu.make_async_remote_copy(
            src_ref=source.at[lead + (source_rows(dr, top, halo), source_cols(dc, left))],
            dst_ref=target.at[lead + (target_rows(dr, dc, halo), target_cols(dc))],
            send_sem=send_sem.at[send, group],
            recv_sem=recv_sem.at[recv, group],
            device_id=device(dz, dr, dc),
            device_id_type=pl.DeviceIdType.MESH,
        )

    held = [(one_pad, one_pad, 2, 0, 0, 0), (two_pad, two_pad, 1, 1, 1, 0)]
    begin = [(x_pad.at[f], x_pad.at[f], 2, 2 + f, 2 + f, 0) for f in range(total)]
    onward = [(out.at[f], x_pad.at[f], 2, 2 + total + f, 2 + f, 1) for f in range(total)]

    def start(stream, allowed, outer):
        for dr, dc in AROUND:
            if dr not in outer:
                continue
            good = exists(dr, dc)
            if allowed is not None:
                good = good & allowed

            @pl.when(good)
            def _():
                remote(*stream, dr, dc).start()

    def settle(sem, view, options, allowed):
        for up in options[0]:
            for side in options[1]:
                shape = view(up, side)
                if shape is None:
                    continue
                good = (ups == up) & (sides == side)
                if allowed is not None:
                    good = good & allowed

                @pl.when(good)
                def _():
                    pltpu.make_async_copy(shape, shape, sem).wait()

    up_options, side_options = neighbours(tile_rows_n), neighbours(tile_cols_n)

    def cut(ref, height, width):
        if height == 0 or width == 0:
            return None
        lead = (slice(None),) * (len(ref.shape) - 3)
        return ref.at[lead + (pl.ds(0, height), pl.ds(0, width))]

    def settle_group(sems, which, stream, group, allowed, centre):
        ref, halo = stream[1], stream[2]
        middle = cols if centre else 0
        if group == MID:
            view = lambda up, side: cut(ref, rows, middle + STRIP * side)
        else:
            view = lambda up, side: cut(ref, halo * up, cols + STRIP * side)
        settle(sems.at[which, group], view, (up_options, side_options), allowed)

    def received(stream, group, allowed=None, centre=False):
        settle_group(recv_sem, stream[4], stream, group, allowed, centre)

    def sent(stream, allowed=None, centre=False):
        for group in (MID, OUTER):
            settle_group(send_sem, stream[3], stream, group, allowed, centre)

    edge = rows // 4

    def tile_copy(f, low, size):
        return pltpu.make_async_remote_copy(
            src_ref=out.at[f, pl.ds(low, size)],
            dst_ref=x_pad.at[f, pl.ds(2 + low, size), pl.ds(EDGE, cols)],
            send_sem=send_sem.at[2 + total + f, MID],
            recv_sem=recv_sem.at[2 + f, MID],
            device_id=device(1, 0, 0),
            device_id_type=pl.DeviceIdType.MESH,
        )

    centre_of = lambda pad, halo: pad.at[:, pl.ds(halo, rows), pl.ds(EDGE, cols)]
    own = local(frames, centre_of(x_pad, 2), 0)
    held_copies = [local(caches.at[0], centre_of(one_pad, 2), 1), local(caches.at[1], centre_of(two_pad, 1), 2)]
    parameters = [
        local(biases_in, biases, 3),
        local(gains_in, gains, 4),
        local(weights_in.at[0], weights.at[0], 5),
        local(weights_in.at[1], weights.at[1], 6),
    ]

    @pl.when(first)
    def _():
        own.start()

    for copy in held_copies + parameters:
        copy.start()

    for pad, halo in ((x_pad, 2), (one_pad, 2), (two_pad, 1)):
        count, height = pad.shape[0], pad.shape[1]
        pad[:, :, 0:EDGE] = jnp.zeros((count, height, EDGE, channels), pad.dtype)
        pad[:, 0:halo, EDGE:] = jnp.zeros((count, halo, cols, channels), pad.dtype)
        pad[:, halo + rows :, EDGE:] = jnp.zeros((count, height - halo - rows, cols, channels), pad.dtype)

    def signal_all(semaphore, steps):
        for dz in steps:
            for dr, dc in AROUND + [(0, 0)]:
                if (dz, dr, dc) == (0, 0, 0):
                    continue

                @pl.when(exists(dr, dc) & (seg + dz >= 0) & (seg + dz < segments))
                def _():
                    pl.semaphore_signal(
                        semaphore, inc=1, device_id=device(dz, dr, dc),
                        device_id_type=pl.DeviceIdType.MESH,
                    )

    plane = (ups + 1) * (sides + 1)
    barrier = pltpu.get_barrier_semaphore()
    signal_all(barrier, (0, 1))
    pl.semaphore_wait(barrier, plane - 1 + plane * number(later))

    @pl.when(first)
    def _():
        own.wait()

    start(begin[0], first, (-1, 1, 0))
    held_copies[0].wait()
    start(held[0], None, (-1, 1, 0))
    held_copies[1].wait()
    start(held[1], None, (-1, 1, 0))
    for f in range(1, total):
        start(begin[f], first, (-1, 1, 0))
    signal_all(ready_sem, (-1,))

    cell = lax.broadcasted_iota(jnp.int32, inside.shape, 0)
    place = cell % pitch
    wrapped = place < EDGE // 2
    cell_row = row * rows + cell // pitch - 1 - number(wrapped)
    cell_col = col * cols + place - EDGE + jnp.where(wrapped, EDGE + cols, 0)
    inside[...] = jnp.where(
        (cell_row >= 0) & (cell_row < rows * tile_rows_n)
        & (cell_col >= 0) & (cell_col < cols * tile_cols_n), 1.0, 0.0,
    )

    def kernel_of(which, *times):
        return jnp.concatenate([weights[which, t] for t in times], axis=1)

    def patches(store, step, parts):
        return jnp.concatenate(
            [
                jnp.concatenate([store[pl.ds(low + dh * step, size), :] for low, size in parts], axis=0)
                for dh in range(TAPS)
            ],
            axis=1,
        )

    def product(store, step, parts, matrix):
        return jnp.dot(patches(store, step, parts), matrix, preferred_element_type=jnp.float32)

    def flat(pad, index, low, high):
        values = pad[index, low:high].astype(jnp.float32)
        return values.reshape((high - low) * pitch, channels)

    def put_all(store, low, values, skip, size):
        for tap, part in enumerate(shifted(values)):
            store[pl.ds(low, size), tap * channels : (tap + 1) * channels] = (
                part[skip : skip + size].astype(jnp.bfloat16)
            )

    def put_tile(store, low, values, height):
        for tap, part in enumerate(shifted(values)):
            part = part[: height * pitch].reshape(height, pitch, channels)[:, EDGE:]
            store[pl.ds(low * cols, height * cols), tap * channels : (tap + 1) * channels] = (
                part.reshape(height * cols, channels).astype(jnp.bfloat16)
            )

    def add_cached(which, store, sums, step, parts):
        bias = biases[which : which + 1]
        older = product(store.at[0], step, parts, kernel_of(which, 0))
        newer = product(store.at[1], step, parts, kernel_of(which, 1, 0))
        at = 0
        for low, size in parts:
            here = slice(at, at + size)
            sums[0, pl.ds(low, size)] = older[here] + newer[here, :channels] + bias
            sums[1, pl.ds(low, size)] = newer[here, channels:] + bias
            at += size

    for copy in parameters:
        copy.wait()

    whole = sum_one.shape[1]
    brim = -(-(3 * pitch + EDGE) // 16) * 16
    rest = (rows - 1) * pitch
    received(held[0], MID)
    for frame in range(2):
        put_all(
            held_taps_one.at[frame], 3 * pitch, flat(one_pad, frame, 3, rows + 2), 0, (rows - 1) * pitch
        )
    low = 3 * pitch
    add_cached(0, held_taps_one, sum_one, pitch, [(low, (rows - 1) * pitch + EDGE - low)])
    received(held[1], MID)
    for frame in range(2):
        put_tile(held_taps_two.at[frame], 2, flat(two_pad, frame, 2, rows + 1), rows - 2)
    add_cached(1, held_taps_two, sum_two, cols, [(2 * cols, (rows - 4) * cols)])

    @pl.when(more & later)
    def _():
        pl.semaphore_wait(ready_sem, plane)

    def held_edges():
        for frame in range(2):
            put_all(held_taps_one.at[frame], 0, flat(one_pad, frame, 0, 5), 0, brim)
            values = flat(one_pad, frame, rows, rows + 5)
            put_all(held_taps_one.at[frame], rows * pitch + EDGE, values, EDGE, 5 * pitch - EDGE)
        add_cached(0, held_taps_one, sum_one, pitch, [(0, brim), (rest, whole - rest)])
        for frame in range(2):
            put_tile(held_taps_two.at[frame], 0, flat(two_pad, frame, 0, 3), 2)
            put_tile(held_taps_two.at[frame], rows, flat(two_pad, frame, rows, rows + 3), 2)
        add_cached(1, held_taps_two, sum_two, cols, [(0, 2 * cols), ((rows - 2) * cols, 2 * cols)])

    def matrix(which, f):
        return kernel_of(which, *((2, 1) if f == 0 else (2,)))

    def act(f, low, high):
        return norm_act(flat(x_pad, f, low, high), gains[0:1])

    def conv_one(f, groups, again=False):
        parts = [
            (low * pitch, whole - low * pitch if low + height == rows + 2 else height * pitch + EDGE)
            for low, height in groups
        ]
        fresh = product(taps_one, pitch, parts, matrix(0, f))
        at = 0
        for (low, height), (base, size) in zip(groups, parts):
            part = pl.ds(base, size)
            hidden = sum_one[f, part] + fresh[at : at + size, :channels]
            if f == 0:
                keep = size if low + height == rows + 2 or again else height * pitch
                sum_one[1, pl.ds(base, keep)] += fresh[at : at + keep, channels:]
            put_tile(taps_two, low, norm_act(hidden, gains[1:2]) * inside[part], height)
            at += size

    def conv_two(f, groups):
        parts = [(low * cols, size * cols) for low, size in groups]
        fresh = product(taps_two, cols, parts, matrix(1, f))
        at = 0
        for low, size in groups:
            here = slice(at, at + size * cols)
            part = pl.ds(low * cols, size * cols)
            branch = sum_two[f, part] + fresh[here, :channels]
            if f == 0:
                sum_two[1, part] += fresh[here, channels:]
            inputs = x_pad[f, 2 + low : 2 + low + size, EDGE:].astype(jnp.float32)
            out[f, low : low + size] = (inputs + branch.reshape(size, cols, channels)).astype(out.dtype)
            at += size * cols

    def send_tile(f, groups):
        @pl.when(more)
        def _():
            for low, size in groups:
                tile_copy(f, low, size).start()

    borders = [(0, edge), (rows - edge, edge)]
    middle = [(edge, rows - 2 * edge)]

    @pl.when(first)
    def _():
        received(begin[0], MID)
        put_all(taps_one, 3 * pitch, act(0, 3, rows + 2), 0, (rows - 1) * pitch)
        conv_one(0, [(3, rows - 4)])
        conv_two(0, middle)
        if segments > 1:
            pl.semaphore_wait(ready_sem, plane)
        send_tile(0, middle)
        for stream in held + begin[:1]:
            received(stream, OUTER)
        held_edges()
        put_all(taps_one, 0, act(0, 0, 5), 0, brim)
        put_all(taps_one, rows * pitch + EDGE, act(0, rows, rows + 5), EDGE, 5 * pitch - EDGE)
        conv_one(0, [(0, 3), (rows - 1, 3)], again=True)
        conv_two(0, borders)

    @pl.when(later)
    def _():
        for stream in held:
            received(stream, OUTER)
        held_edges()
        received(onward[0], OUTER)
        received(onward[0], MID, None, True)
        put_all(taps_one, 0, act(0, 0, rows + 5), 0, (rows + 5) * pitch)
        conv_one(0, [(0, edge + 2), (rows - edge, edge + 2)])
        conv_two(0, borders)

    start(onward[0], more, (-1, 1))
    send_tile(0, borders)

    @pl.when(later)
    def _():
        conv_one(0, [(edge + 2, rows - 2 * edge - 2)])
        conv_two(0, middle)
        send_tile(0, middle)

    start(onward[0], more, (0,))

    for f in range(1, total):
        for group in (MID, OUTER):
            received(begin[f], group, first)
            received(onward[f], group, later, group == MID)
        put_all(taps_one, 0, act(f, 0, rows + 5), 0, (rows + 5) * pitch)
        conv_one(f, [(0, rows + 2)])
        conv_two(f, [(0, rows)])
        sent(onward[f - 1], more, True)
        start(onward[f], more, (-1, 1))
        send_tile(f, borders + middle)
        start(onward[f], more, (0,))

    for stream in held:
        sent(stream)
    for f in range(total):
        sent(begin[f], first)
    sent(onward[total - 1], more, True)


def solution(mesh):
    counts = tuple(mesh.shape[name] for name in ("segment", "row", "col"))

    def on_device(frames, caches, weights, biases, gains):
        total, rows, cols, channels = frames.shape
        pitch = cols + EDGE
        whole = -(-((rows + 2) * pitch + EDGE) // 16) * 16
        bf16, f32 = jnp.bfloat16, jnp.float32
        vmem = pl.BlockSpec(memory_space=pltpu.VMEM)
        taps = weights.reshape(2, TAPS, TAPS * TAPS * channels, channels)
        result = pl.pallas_call(
            functools.partial(kernel, counts),
            out_shape=pltpu.VMEM(frames.shape, bf16),
            in_specs=[pl.BlockSpec(memory_space=pl.ANY)] * 5,
            out_specs=vmem,
            scratch_shapes=[
                pltpu.VMEM(taps.shape, bf16),
                pltpu.VMEM(biases.shape[1:], f32),
                pltpu.VMEM(gains.shape[1:], f32),
                pltpu.VMEM((total, rows + 5, pitch, channels), bf16),
                pltpu.VMEM((2, rows + 5, pitch, channels), bf16),
                pltpu.VMEM((2, rows + 3, pitch, channels), bf16),
                pltpu.VMEM(((rows + 5) * pitch, TAPS * channels), bf16),
                pltpu.VMEM(((rows + 2) * cols, TAPS * channels), bf16),
                pltpu.VMEM((2, (rows + 5) * pitch, TAPS * channels), bf16),
                pltpu.VMEM((2, (rows + 2) * cols, TAPS * channels), bf16),
                pltpu.VMEM((total, whole, channels), f32),
                pltpu.VMEM((total, rows * cols, channels), f32),
                pltpu.VMEM((whole, channels), f32),
                pltpu.SemaphoreType.DMA((2 + 2 * total, 2)),
                pltpu.SemaphoreType.DMA((2 + total, 2)),
                pltpu.SemaphoreType.DMA((7,)),
                pltpu.SemaphoreType.REGULAR,
            ],
            compiler_params=pltpu.CompilerParams(collective_id=0, has_side_effects=True),
        )(frames, caches[0], taps, biases[0], gains[0])
        return result[None]

    in_specs = (
        P(None, "row", "col", None),
        P("segment", None, None, "row", "col", None),
        P("segment", None, None, None, None, None, None),
        P("segment", None, None),
        P("segment", None, None),
    )
    out_specs = P("segment", None, "row", "col", None)
    return jax.shard_map(
        on_device, mesh=mesh, in_specs=in_specs, out_specs=out_specs, check_vma=False
    )
```

```python
import functools

import jax
import jax.numpy as jnp
from jax import lax
from jax.experimental import pallas as pl
from jax.experimental.pallas import tpu as pltpu
from jax.sharding import PartitionSpec as P

EDGE = 8
STRIP = 2
TAPS = 3
AROUND = [(dr, dc) for dr in (-1, 1, 0) for dc in (0, -1, 1) if (dr, dc) != (0, 0)]
MID, OUTER = 0, 1


def neighbours(count):
    return {1: (0,), 2: (1,)}.get(count, (1, 2))


def norm_act(values, gain_row):
    scale = lax.rsqrt(jnp.mean(values * values, axis=-1, keepdims=True) + 1e-06)
    half = 0.5 * (values * scale * gain_row)
    return half * jnp.tanh(half) + half


def shifted(values):
    size = values.shape[0]
    return pltpu.roll(values, 1, 0), values, pltpu.roll(values, size - 1, 0)


def kernel(
    counts,
    frames, caches, weights_in, biases_in, gains_in,
    out,
    weights, biases, gains, x_pad, one_pad, two_pad, taps_one, taps_two,
    held_taps_one, held_taps_two, sum_one, sum_two, inside,
    send_sem, recv_sem, local_sem, ready_sem,
):
    segments, tile_rows_n, tile_cols_n = counts
    seg, row, col = (lax.axis_index(name) for name in ("segment", "row", "col"))
    total, rows, cols, channels = frames.shape
    pitch = cols + EDGE
    first = seg == 0
    later = seg > 0
    more = seg < segments - 1

    def exists(dr, dc):
        r, c = row + dr, col + dc
        return (r >= 0) & (r < tile_rows_n) & (c >= 0) & (c < tile_cols_n)

    def device(dz, dr, dc):
        return {"segment": seg + dz, "row": row + dr, "col": col + dc}

    def number(flag):
        return flag.astype(jnp.int32)

    ups = number(row > 0) + number(row < tile_rows_n - 1)
    sides = number(col > 0) + number(col < tile_cols_n - 1)

    def local(source, target, which):
        return pltpu.make_async_copy(source, target, local_sem.at[which])

    def source_rows(dr, base, halo):
        if dr == 0:
            return pl.ds(base, rows)
        return pl.ds(base if dr < 0 else base + rows - halo, halo)

    def source_cols(dc, base):
        if dc == 0:
            return pl.ds(base, cols)
        return pl.ds(base if dc < 0 else base + cols - STRIP, STRIP)

    def target_rows(dr, dc, halo):
        skip = 1 if dc < 0 else 0
        if dr == 0:
            return pl.ds(halo + skip, rows)
        return pl.ds((halo + rows if dr < 0 else 0) + skip, halo)

    def target_cols(dc):
        if dc == 0:
            return pl.ds(EDGE, cols)
        return pl.ds(0, STRIP) if dc < 0 else pl.ds(EDGE - STRIP, STRIP)

    def remote(source, target, halo, send, recv, dz, dr, dc):
        top, left = (0, 0) if dz else (halo, EDGE)
        lead = (slice(None),) * (len(source.shape) - 3)
        group = OUTER if dr else MID
        return pltpu.make_async_remote_copy(
            src_ref=source.at[lead + (source_rows(dr, top, halo), source_cols(dc, left))],
            dst_ref=target.at[lead + (target_rows(dr, dc, halo), target_cols(dc))],
            send_sem=send_sem.at[send, group],
            recv_sem=recv_sem.at[recv, group],
            device_id=device(dz, dr, dc),
            device_id_type=pl.DeviceIdType.MESH,
        )

    held = [(one_pad, one_pad, 2, 0, 0, 0), (two_pad, two_pad, 1, 1, 1, 0)]
    begin = [(x_pad.at[f], x_pad.at[f], 2, 2 + f, 2 + f, 0) for f in range(total)]
    onward = [(out.at[f], x_pad.at[f], 2, 2 + total + f, 2 + f, 1) for f in range(total)]

    def start(stream, allowed, outer):
        for dr, dc in AROUND:
            if dr not in outer:
                continue
            good = exists(dr, dc)
            if allowed is not True:
                good = good & allowed

            @pl.when(good)
            def _():
                remote(*stream, dr, dc).start()

    def settle(sem, view, options, allowed):
        for up in options[0]:
            for side in options[1]:
                shape = view(up, side)
                if shape is None:
                    continue
                good = (ups == up) & (sides == side)
                if allowed is not None:
                    good = good & allowed

                @pl.when(good)
                def _():
                    pltpu.make_async_copy(shape, shape, sem).wait()

    up_options, side_options = neighbours(tile_rows_n), neighbours(tile_cols_n)

    def cut(ref, height, width):
        if height == 0 or width == 0:
            return None
        lead = (slice(None),) * (len(ref.shape) - 3)
        return ref.at[lead + (pl.ds(0, height), pl.ds(0, width))]

    def settle_group(sems, which, stream, group, allowed, centre):
        ref, halo = stream[1], stream[2]
        middle = cols if centre else 0
        if group == MID:
            view = lambda up, side: cut(ref, rows, middle + STRIP * side)
        else:
            view = lambda up, side: cut(ref, halo * up, cols + STRIP * side)
        settle(sems.at[which, group], view, (up_options, side_options), allowed)

    def received(stream, group, allowed=None, centre=False):
        settle_group(recv_sem, stream[4], stream, group, allowed, centre)

    def sent(stream, allowed=None, centre=False, groups=(MID, OUTER)):
        for group in groups:
            settle_group(send_sem, stream[3], stream, group, allowed, centre)

    edge = rows // 4

    def tile_copy(f, low, size):
        return pltpu.make_async_remote_copy(
            src_ref=out.at[f, pl.ds(low, size)],
            dst_ref=x_pad.at[f, pl.ds(2 + low, size), pl.ds(EDGE, cols)],
            send_sem=send_sem.at[2 + total + f, MID],
            recv_sem=recv_sem.at[2 + f, MID],
            device_id=device(1, 0, 0),
            device_id_type=pl.DeviceIdType.MESH,
        )

    centre_of = lambda pad, halo: pad.at[:, pl.ds(halo, rows), pl.ds(EDGE, cols)]
    own = local(frames, centre_of(x_pad, 2), 0)
    held_copies = [local(caches.at[0], centre_of(one_pad, 2), 1), local(caches.at[1], centre_of(two_pad, 1), 2)]
    parameters = [
        local(biases_in, biases, 3),
        local(gains_in, gains, 4),
        local(weights_in.at[0], weights.at[0], 5),
        local(weights_in.at[1], weights.at[1], 6),
    ]

    @pl.when(first)
    def _():
        own.start()

    for copy in held_copies + parameters:
        copy.start()

    for pad, halo in ((x_pad, 2), (one_pad, 2), (two_pad, 1)):
        count, height = pad.shape[0], pad.shape[1]
        pad[:, :, 0:EDGE] = jnp.zeros((count, height, EDGE, channels), pad.dtype)
        pad[:, 0:halo, EDGE:] = jnp.zeros((count, halo, cols, channels), pad.dtype)
        pad[:, halo + rows :, EDGE:] = jnp.zeros((count, height - halo - rows, cols, channels), pad.dtype)

    def signal_all(semaphore, steps):
        for dz in steps:
            for dr, dc in AROUND + [(0, 0)]:
                if (dz, dr, dc) == (0, 0, 0):
                    continue

                @pl.when(exists(dr, dc) & (seg + dz >= 0) & (seg + dz < segments))
                def _():
                    pl.semaphore_signal(
                        semaphore, inc=1, device_id=device(dz, dr, dc),
                        device_id_type=pl.DeviceIdType.MESH,
                    )

    plane = (ups + 1) * (sides + 1)
    barrier = pltpu.get_barrier_semaphore()
    signal_all(barrier, (0, 1))
    pl.semaphore_wait(barrier, plane - 1 + plane * number(later))

    @pl.when(first)
    def _():
        own.wait()

    for copy in held_copies:
        copy.wait()
    early = [(begin[0], first), (held[0], True), (held[1], True)]
    even = row % 2 == 0
    for stream, allowed in early:
        start(stream, even & allowed, (-1,))
        start(stream, ~even & allowed, (1,))
    for stream, allowed in early:
        start(stream, allowed, (0,))
    for stream, allowed in early:
        start(stream, even & allowed, (1,))
        start(stream, ~even & allowed, (-1,))
    for f in range(1, total):
        start(begin[f], first, (-1, 1, 0))
    signal_all(ready_sem, (-1,))

    cell = lax.broadcasted_iota(jnp.int32, inside.shape, 0)
    place = cell % pitch
    wrapped = place < EDGE // 2
    cell_row = row * rows + cell // pitch - 1 - number(wrapped)
    cell_col = col * cols + place - EDGE + jnp.where(wrapped, EDGE + cols, 0)
    inside[...] = jnp.where(
        (cell_row >= 0) & (cell_row < rows * tile_rows_n)
        & (cell_col >= 0) & (cell_col < cols * tile_cols_n), 1.0, 0.0,
    )

    def kernel_of(which, *times):
        return jnp.concatenate([weights[which, t] for t in times], axis=1)

    def patches(store, step, parts):
        return jnp.concatenate(
            [
                jnp.concatenate([store[pl.ds(low + dh * step, size), :] for low, size in parts], axis=0)
                for dh in range(TAPS)
            ],
            axis=1,
        )

    def product(store, step, parts, matrix):
        return jnp.dot(patches(store, step, parts), matrix, preferred_element_type=jnp.float32)

    def flat(pad, index, low, high):
        values = pad[index, low:high].astype(jnp.float32)
        return values.reshape((high - low) * pitch, channels)

    def put_all(store, low, values, skip, size):
        for tap, part in enumerate(shifted(values)):
            store[pl.ds(low, size), tap * channels : (tap + 1) * channels] = (
                part[skip : skip + size].astype(jnp.bfloat16)
            )

    def put_tile(store, low, values, height):
        for tap, part in enumerate(shifted(values)):
            part = part[: height * pitch].reshape(height, pitch, channels)[:, EDGE:]
            store[pl.ds(low * cols, height * cols), tap * channels : (tap + 1) * channels] = (
                part.reshape(height * cols, channels).astype(jnp.bfloat16)
            )

    def add_cached(which, store, sums, step, parts):
        bias = biases[which : which + 1]
        older = product(store.at[0], step, parts, kernel_of(which, 0))
        newer = product(store.at[1], step, parts, kernel_of(which, 1, 0))
        at = 0
        for low, size in parts:
            here = slice(at, at + size)
            sums[0, pl.ds(low, size)] = older[here] + newer[here, :channels] + bias
            sums[1, pl.ds(low, size)] = newer[here, channels:] + bias
            at += size

    for copy in parameters:
        copy.wait()

    whole = sum_one.shape[1]
    brim = -(-(3 * pitch + EDGE) // 16) * 16
    rest = (rows - 1) * pitch
    received(held[0], MID)
    for frame in range(2):
        put_all(
            held_taps_one.at[frame], 3 * pitch, flat(one_pad, frame, 3, rows + 2), 0, (rows - 1) * pitch
        )
    low = 3 * pitch
    add_cached(0, held_taps_one, sum_one, pitch, [(low, (rows - 1) * pitch + EDGE - low)])
    received(held[1], MID)
    for frame in range(2):
        put_tile(held_taps_two.at[frame], 2, flat(two_pad, frame, 2, rows + 1), rows - 2)
    add_cached(1, held_taps_two, sum_two, cols, [(2 * cols, (rows - 4) * cols)])

    @pl.when(more & later)
    def _():
        pl.semaphore_wait(ready_sem, plane)

    def held_edge_one():
        for frame in range(2):
            put_all(held_taps_one.at[frame], 0, flat(one_pad, frame, 0, 5), 0, brim)
            values = flat(one_pad, frame, rows, rows + 5)
            put_all(held_taps_one.at[frame], rows * pitch + EDGE, values, EDGE, 5 * pitch - EDGE)
        add_cached(0, held_taps_one, sum_one, pitch, [(0, brim), (rest, whole - rest)])

    def held_edge_two():
        for frame in range(2):
            put_tile(held_taps_two.at[frame], 0, flat(two_pad, frame, 0, 3), 2)
            put_tile(held_taps_two.at[frame], rows, flat(two_pad, frame, rows, rows + 3), 2)
        add_cached(1, held_taps_two, sum_two, cols, [(0, 2 * cols), ((rows - 2) * cols, 2 * cols)])

    def matrix(which, f):
        return kernel_of(which, *((2, 1) if f == 0 else (2,)))

    def act(f, low, high):
        return norm_act(flat(x_pad, f, low, high), gains[0:1])

    def act_split(f, at):
        put_all(taps_one, 0, act(f, 0, at + 1), 0, at * pitch)
        put_all(taps_one, at * pitch, act(f, at - 1, rows + 5), pitch, (rows + 5 - at) * pitch)

    def spans_one(groups):
        return [
            (low * pitch, whole - low * pitch if low + height == rows + 2 else height * pitch + EDGE)
            for low, height in groups
        ]

    def spans_two(groups):
        return [(low * cols, size * cols) for low, size in groups]

    def multiply_one(f, groups):
        return product(taps_one, pitch, spans_one(groups), matrix(0, f))

    def multiply_two(f, groups):
        return product(taps_two, cols, spans_two(groups), matrix(1, f))

    def finish_one(f, groups, fresh, again=False):
        at = 0
        for (low, height), (base, size) in zip(groups, spans_one(groups)):
            part = pl.ds(base, size)
            hidden = sum_one[f, part] + fresh[at : at + size, :channels]
            if f == 0:
                keep = size if low + height == rows + 2 or again else height * pitch
                sum_one[1, pl.ds(base, keep)] += fresh[at : at + keep, channels:]
            put_tile(taps_two, low, norm_act(hidden, gains[1:2]) * inside[part], height)
            at += size

    def finish_two(f, groups, fresh):
        at = 0
        for (low, size), (base, count) in zip(groups, spans_two(groups)):
            here, part = slice(at, at + count), pl.ds(base, count)
            branch = sum_two[f, part] + fresh[here, :channels]
            if f == 0:
                sum_two[1, part] += fresh[here, channels:]
            inputs = x_pad[f, 2 + low : 2 + low + size, EDGE:].astype(jnp.float32)
            out[f, low : low + size] = (inputs + branch.reshape(size, cols, channels)).astype(out.dtype)
            at += count

    def stage(f, ones, twos):
        firsts = [multiply_one(f, groups) for groups in ones]
        for groups, fresh in zip(ones, firsts):
            finish_one(f, groups, fresh)
        seconds = [multiply_two(f, groups) for groups in twos]
        for groups, fresh in zip(twos, seconds):
            finish_two(f, groups, fresh)

    def send_tile(f, groups):
        @pl.when(more)
        def _():
            for low, size in groups:
                tile_copy(f, low, size).start()

    borders = [(0, edge), (rows - edge, edge)]
    middle = [(edge, rows - 2 * edge)]

    @pl.when(first)
    def _():
        received(begin[0], MID)
        put_all(taps_one, 3 * pitch, act(0, 3, rows + 2), 0, (rows - 1) * pitch)
        stage(0, [[(3, rows - 4)]], [middle])
        if segments > 1:
            pl.semaphore_wait(ready_sem, plane)
        send_tile(0, middle)
        for stream in held + begin[:1]:
            received(stream, OUTER)
        put_all(taps_one, 0, act(0, 0, 5), 0, brim)
        put_all(taps_one, rows * pitch + EDGE, act(0, rows, rows + 5), EDGE, 5 * pitch - EDGE)
        held_edge_one()
        ends = [(0, 3), (rows - 1, 3)]
        fresh = multiply_one(0, ends)
        held_edge_two()
        finish_one(0, ends, fresh, again=True)
        finish_two(0, borders, multiply_two(0, borders))
        start(onward[0], more, (-1, 1))
        send_tile(0, borders)

    @pl.when(later)
    def _():
        received(held[0], OUTER)
        held_edge_one()
        received(held[1], OUTER)
        held_edge_two()
        received(onward[0], OUTER)
        received(onward[0], MID, None, True)

    @pl.when(later & more)
    def _():
        act_split(0, rows // 2 + 2)
        tops, lows, mids = [(0, edge + 2)], [(rows - edge, edge + 2)], [(edge + 2, rows - 2 * edge - 2)]
        top, low, mid = (multiply_one(0, groups) for groups in (tops, lows, mids))
        finish_one(0, tops, top)
        top = multiply_two(0, borders[:1])
        finish_one(0, lows, low)
        finish_one(0, mids, mid)
        finish_two(0, borders[:1], top)
        start(onward[0], True, (-1,))
        send_tile(0, borders[:1])
        low, mid = multiply_two(0, borders[1:]), multiply_two(0, middle)
        finish_two(0, borders[1:], low)
        start(onward[0], True, (1,))
        send_tile(0, borders[1:])
        finish_two(0, middle, mid)
        send_tile(0, middle)

    half = rows // 2
    halves = [[(0, half)], [(half, rows + 2 - half)]], [[(0, half - 2)], [(half - 2, rows + 2 - half)]]

    @pl.when(later & ~more)
    def _():
        act_split(0, half + 3)
        stage(0, *halves)

    start(onward[0], more, (0,))

    for f in range(1, total):
        for group in (MID, OUTER):
            received(begin[f], group, first)
            received(onward[f], group, later, group == MID)
        act_split(f, half + 3)
        stage(f, *halves)
        sent(onward[f - 1], more, True, (OUTER,))
        start(onward[f], more, (-1, 1))
        send_tile(f, borders + middle)
        start(onward[f], more, (0,))

    for stream in held:
        sent(stream)
    for f in range(total):
        sent(begin[f], first)
        sent(onward[f], more, True, (MID,) if f + 1 < total else (MID, OUTER))


def solution(mesh):
    counts = tuple(mesh.shape[name] for name in ("segment", "row", "col"))

    def on_device(frames, caches, weights, biases, gains):
        total, rows, cols, channels = frames.shape
        pitch = cols + EDGE
        whole = -(-((rows + 2) * pitch + EDGE) // 16) * 16
        bf16, f32 = jnp.bfloat16, jnp.float32
        vmem = pl.BlockSpec(memory_space=pltpu.VMEM)
        taps = weights.reshape(2, TAPS, TAPS * TAPS * channels, channels)
        result = pl.pallas_call(
            functools.partial(kernel, counts),
            out_shape=pltpu.VMEM(frames.shape, bf16),
            in_specs=[pl.BlockSpec(memory_space=pl.ANY)] * 5,
            out_specs=vmem,
            scratch_shapes=[
                pltpu.VMEM(taps.shape, bf16),
                pltpu.VMEM(biases.shape[1:], f32),
                pltpu.VMEM(gains.shape[1:], f32),
                pltpu.VMEM((total, rows + 5, pitch, channels), bf16),
                pltpu.VMEM((2, rows + 5, pitch, channels), bf16),
                pltpu.VMEM((2, rows + 3, pitch, channels), bf16),
                pltpu.VMEM(((rows + 5) * pitch, TAPS * channels), bf16),
                pltpu.VMEM(((rows + 2) * cols, TAPS * channels), bf16),
                pltpu.VMEM((2, (rows + 5) * pitch, TAPS * channels), bf16),
                pltpu.VMEM((2, (rows + 2) * cols, TAPS * channels), bf16),
                pltpu.VMEM((total, whole, channels), f32),
                pltpu.VMEM((total, rows * cols, channels), f32),
                pltpu.VMEM((whole, channels), f32),
                pltpu.SemaphoreType.DMA((2 + 2 * total, 2)),
                pltpu.SemaphoreType.DMA((2 + total, 2)),
                pltpu.SemaphoreType.DMA((7,)),
                pltpu.SemaphoreType.REGULAR,
            ],
            compiler_params=pltpu.CompilerParams(collective_id=0, has_side_effects=True),
        )(frames, caches[0], taps, biases[0], gains[0])
        return result[None]

    in_specs = (
        P(None, "row", "col", None),
        P("segment", None, None, "row", "col", None),
        P("segment", None, None, None, None, None, None),
        P("segment", None, None),
        P("segment", None, None),
    )
    out_specs = P("segment", None, "row", "col", None)
    return jax.shard_map(
        on_device, mesh=mesh, in_specs=in_specs, out_specs=out_specs, check_vma=False
    )
```

```python
import functools

import jax
import jax.numpy as jnp
from jax import lax
from jax.experimental import pallas as pl
from jax.experimental.pallas import tpu as pltpu
from jax.sharding import PartitionSpec as P

EDGE = 8
STRIP = 2
TAPS = 3
AROUND = [(dr, dc) for dr in (-1, 1, 0) for dc in (0, -1, 1) if (dr, dc) != (0, 0)]
MID, OUTER = 0, 1


def neighbours(count):
    return {1: (0,), 2: (1,)}.get(count, (1, 2))


def norm_act(values, gain_row):
    scale = lax.rsqrt(jnp.mean(values * values, axis=-1, keepdims=True) + 1e-06)
    half = 0.5 * (values * scale * gain_row)
    return half * jnp.tanh(half) + half


def shifted(values):
    size = values.shape[0]
    return pltpu.roll(values, 1, 0), values, pltpu.roll(values, size - 1, 0)


def kernel(
    counts,
    frames, caches, weights_in, biases_in, gains_in,
    out,
    weights, biases, gains, x_pad, one_pad, two_pad, taps_one, taps_two,
    held_taps_one, held_taps_two, sum_one, sum_two, inside,
    send_sem, recv_sem, local_sem, ready_sem,
):
    segments, tile_rows_n, tile_cols_n = counts
    seg, row, col = (lax.axis_index(name) for name in ("segment", "row", "col"))
    total, rows, cols, channels = frames.shape
    pitch = cols + EDGE
    first = seg == 0
    later = seg > 0
    more = seg < segments - 1

    def exists(dr, dc):
        r, c = row + dr, col + dc
        return (r >= 0) & (r < tile_rows_n) & (c >= 0) & (c < tile_cols_n)

    def device(dz, dr, dc):
        return {"segment": seg + dz, "row": row + dr, "col": col + dc}

    def number(flag):
        return flag.astype(jnp.int32)

    ups = number(row > 0) + number(row < tile_rows_n - 1)
    sides = number(col > 0) + number(col < tile_cols_n - 1)

    def local(source, target, which):
        return pltpu.make_async_copy(source, target, local_sem.at[which])

    def source_rows(dr, base, halo):
        if dr == 0:
            return pl.ds(base, rows)
        return pl.ds(base if dr < 0 else base + rows - halo, halo)

    def source_cols(dc, base):
        if dc == 0:
            return pl.ds(base, cols)
        return pl.ds(base if dc < 0 else base + cols - STRIP, STRIP)

    def target_rows(dr, dc, halo):
        skip = 1 if dc < 0 else 0
        if dr == 0:
            return pl.ds(halo + skip, rows)
        return pl.ds((halo + rows if dr < 0 else 0) + skip, halo)

    def target_cols(dc):
        if dc == 0:
            return pl.ds(EDGE, cols)
        return pl.ds(0, STRIP) if dc < 0 else pl.ds(EDGE - STRIP, STRIP)

    def remote(source, target, halo, send, recv, dz, dr, dc):
        top, left = (0, 0) if dz else (halo, EDGE)
        lead = (slice(None),) * (len(source.shape) - 3)
        group = OUTER if dr else MID
        return pltpu.make_async_remote_copy(
            src_ref=source.at[lead + (source_rows(dr, top, halo), source_cols(dc, left))],
            dst_ref=target.at[lead + (target_rows(dr, dc, halo), target_cols(dc))],
            send_sem=send_sem.at[send, group],
            recv_sem=recv_sem.at[recv, group],
            device_id=device(dz, dr, dc),
            device_id_type=pl.DeviceIdType.MESH,
        )

    held = [(one_pad, one_pad, 2, 0, 0, 0), (two_pad, two_pad, 1, 0, 1, 0)]
    begin = [(x_pad.at[f], x_pad.at[f], 2, 0, 2 + f, 0) for f in range(total)]
    onward = [(out.at[f], x_pad.at[f], 2, 1 + f, 2 + f, 1) for f in range(total)]

    def start(stream, allowed, outer):
        for dr, dc in AROUND:
            if dr not in outer:
                continue
            good = exists(dr, dc)
            if allowed is not True:
                good = good & allowed

            @pl.when(good)
            def _():
                remote(*stream, dr, dc).start()

    def settle(sem, view, options, allowed):
        for up in options[0]:
            for side in options[1]:
                shape = view(up, side)
                if shape is None:
                    continue
                good = (ups == up) & (sides == side)
                if allowed is not None:
                    good = good & allowed

                @pl.when(good)
                def _():
                    pltpu.make_async_copy(shape, shape, sem).wait()

    up_options, side_options = neighbours(tile_rows_n), neighbours(tile_cols_n)

    def cut(ref, height, width):
        if height == 0 or width == 0:
            return None
        lead = (slice(None),) * (len(ref.shape) - 3)
        return ref.at[lead + (pl.ds(0, height), pl.ds(0, width))]

    def settle_group(sems, which, stream, group, allowed, centre):
        ref, halo = stream[1], stream[2]
        middle = cols if centre else 0
        if group == MID:
            view = lambda up, side: cut(ref, rows, middle + STRIP * side)
        else:
            view = lambda up, side: cut(ref, halo * up, cols + STRIP * side)
        settle(sems.at[which, group], view, (up_options, side_options), allowed)

    def received(stream, group, allowed=None, centre=False):
        settle_group(recv_sem, stream[4], stream, group, allowed, centre)

    def sent(stream, allowed=None, centre=False, groups=(MID, OUTER)):
        for group in groups:
            settle_group(send_sem, stream[3], stream, group, allowed, centre)

    edge = rows // 4

    def tile_copy(f, low, size):
        return pltpu.make_async_remote_copy(
            src_ref=out.at[f, pl.ds(low, size)],
            dst_ref=x_pad.at[f, pl.ds(2 + low, size), pl.ds(EDGE, cols)],
            send_sem=send_sem.at[1 + f, MID],
            recv_sem=recv_sem.at[2 + f, MID],
            device_id=device(1, 0, 0),
            device_id_type=pl.DeviceIdType.MESH,
        )

    centre_of = lambda pad, halo: pad.at[:, pl.ds(halo, rows), pl.ds(EDGE, cols)]
    own = local(frames, centre_of(x_pad, 2), 0)
    held_copies = [local(caches.at[0], centre_of(one_pad, 2), 1), local(caches.at[1], centre_of(two_pad, 1), 1)]
    parameters = [local(biases_in, biases, 2), local(gains_in, gains, 2), local(weights_in, weights, 3)]
    few = sum_one.at[0, pl.ds(0, biases.shape[0] + gains.shape[0])]

    @pl.when(first)
    def _():
        own.start()

    for copy in held_copies + parameters:
        copy.start()

    for pad, halo in ((x_pad, 2), (one_pad, 2), (two_pad, 1)):
        count, height = pad.shape[0], pad.shape[1]
        pad[:, :, 0:EDGE] = jnp.zeros((count, height, EDGE, channels), pad.dtype)
        pad[:, 0:halo, EDGE:] = jnp.zeros((count, halo, cols, channels), pad.dtype)
        pad[:, halo + rows :, EDGE:] = jnp.zeros((count, height - halo - rows, cols, channels), pad.dtype)

    def signal_all(semaphore, steps):
        for dz in steps:
            for dr, dc in AROUND + [(0, 0)]:
                if (dz, dr, dc) == (0, 0, 0):
                    continue

                @pl.when(exists(dr, dc) & (seg + dz >= 0) & (seg + dz < segments))
                def _():
                    pl.semaphore_signal(
                        semaphore, inc=1, device_id=device(dz, dr, dc),
                        device_id_type=pl.DeviceIdType.MESH,
                    )

    plane = (ups + 1) * (sides + 1)
    barrier = pltpu.get_barrier_semaphore()
    signal_all(barrier, (0, 1))
    pl.semaphore_wait(barrier, plane - 1 + plane * number(later))

    @pl.when(first)
    def _():
        own.wait()

    local(caches, caches, 1).wait()
    even = row % 2 == 0
    for early in ([(held[0], True), (begin[0], first)], [(held[1], True)]):
        for stream, allowed in early:
            start(stream, even & allowed, (-1,))
            start(stream, ~even & allowed, (1,))
        for stream, allowed in early:
            start(stream, allowed, (0,))
        for stream, allowed in early:
            start(stream, even & allowed, (1,))
            start(stream, ~even & allowed, (-1,))
    for f in range(1, total):
        start(begin[f], first, (-1, 1, 0))
    signal_all(ready_sem, (-1,))

    cell = lax.broadcasted_iota(jnp.int32, inside.shape, 0)
    place = cell % pitch
    wrapped = place < EDGE // 2
    cell_row = row * rows + cell // pitch - 1 - number(wrapped)
    cell_col = col * cols + place - EDGE + jnp.where(wrapped, EDGE + cols, 0)
    inside[...] = jnp.where(
        (cell_row >= 0) & (cell_row < rows * tile_rows_n)
        & (cell_col >= 0) & (cell_col < cols * tile_cols_n), 1.0, 0.0,
    )

    def kernel_of(which, *times):
        return jnp.concatenate([weights[which, t] for t in times], axis=1)

    def patches(store, step, parts):
        return jnp.concatenate(
            [
                jnp.concatenate([store[pl.ds(low + dh * step, size), :] for low, size in parts], axis=0)
                for dh in range(TAPS)
            ],
            axis=1,
        )

    def product(store, step, parts, matrix):
        return jnp.dot(patches(store, step, parts), matrix, preferred_element_type=jnp.float32)

    def flat(pad, index, low, high):
        values = pad[index, low:high].astype(jnp.float32)
        return values.reshape((high - low) * pitch, channels)

    def put_all(store, low, values, skip, size):
        for tap, part in enumerate(shifted(values)):
            store[pl.ds(low, size), tap * channels : (tap + 1) * channels] = (
                part[skip : skip + size].astype(jnp.bfloat16)
            )

    def put_tile(store, low, values, height):
        for tap, part in enumerate(shifted(values)):
            part = part[: height * pitch].reshape(height, pitch, channels)[:, EDGE:]
            store[pl.ds(low * cols, height * cols), tap * channels : (tap + 1) * channels] = (
                part.reshape(height * cols, channels).astype(jnp.bfloat16)
            )

    def add_cached(which, store, sums, step, parts):
        bias = biases[which : which + 1]
        older = product(store.at[0], step, parts, kernel_of(which, 0))
        newer = product(store.at[1], step, parts, kernel_of(which, 1, 0))
        at = 0
        for low, size in parts:
            here = slice(at, at + size)
            sums[0, pl.ds(low, size)] = older[here] + newer[here, :channels] + bias
            sums[1, pl.ds(low, size)] = newer[here, channels:] + bias
            at += size

    local(few, few, 2).wait()
    parameters[-1].wait()

    whole = sum_one.shape[1]
    brim = -(-(3 * pitch + EDGE) // 16) * 16
    rest = (rows - 1) * pitch
    received(held[0], MID)
    for frame in range(2):
        put_all(
            held_taps_one.at[frame], 3 * pitch, flat(one_pad, frame, 3, rows + 2), 0, (rows - 1) * pitch
        )
    low = 3 * pitch
    add_cached(0, held_taps_one, sum_one, pitch, [(low, (rows - 1) * pitch + EDGE - low)])
    received(held[1], MID)
    for frame in range(2):
        put_tile(held_taps_two.at[frame], 2, flat(two_pad, frame, 2, rows + 1), rows - 2)
    add_cached(1, held_taps_two, sum_two, cols, [(2 * cols, (rows - 4) * cols)])

    @pl.when(more & later)
    def _():
        pl.semaphore_wait(ready_sem, plane)

    def held_edge_one():
        for frame in range(2):
            put_all(held_taps_one.at[frame], 0, flat(one_pad, frame, 0, 5), 0, brim)
            values = flat(one_pad, frame, rows, rows + 5)
            put_all(held_taps_one.at[frame], rows * pitch + EDGE, values, EDGE, 5 * pitch - EDGE)
        add_cached(0, held_taps_one, sum_one, pitch, [(0, brim), (rest, whole - rest)])

    def held_edge_two():
        for frame in range(2):
            put_tile(held_taps_two.at[frame], 0, flat(two_pad, frame, 0, 3), 2)
            put_tile(held_taps_two.at[frame], rows, flat(two_pad, frame, rows, rows + 3), 2)
        add_cached(1, held_taps_two, sum_two, cols, [(0, 2 * cols), ((rows - 2) * cols, 2 * cols)])

    def matrix(which, f):
        return kernel_of(which, *((2, 1) if f == 0 else (2,)))

    def act(f, low, high):
        return norm_act(flat(x_pad, f, low, high), gains[0:1])

    def act_split(f, at):
        put_all(taps_one, 0, act(f, 0, at + 1), 0, at * pitch)
        put_all(taps_one, at * pitch, act(f, at - 1, rows + 5), pitch, (rows + 5 - at) * pitch)

    def spans_one(groups):
        return [
            (low * pitch, whole - low * pitch if low + height == rows + 2 else height * pitch + EDGE)
            for low, height in groups
        ]

    def spans_two(groups):
        return [(low * cols, size * cols) for low, size in groups]

    def multiply_one(f, groups):
        return product(taps_one, pitch, spans_one(groups), matrix(0, f))

    def multiply_two(f, groups):
        return product(taps_two, cols, spans_two(groups), matrix(1, f))

    def finish_one(f, groups, fresh, again=False):
        at = 0
        for (low, height), (base, size) in zip(groups, spans_one(groups)):
            part = pl.ds(base, size)
            hidden = sum_one[f, part] + fresh[at : at + size, :channels]
            if f == 0:
                keep = size if low + height == rows + 2 or again else height * pitch
                sum_one[1, pl.ds(base, keep)] += fresh[at : at + keep, channels:]
            put_tile(taps_two, low, norm_act(hidden, gains[1:2]) * inside[part], height)
            at += size

    def finish_two(f, groups, fresh):
        at = 0
        for (low, size), (base, count) in zip(groups, spans_two(groups)):
            here, part = slice(at, at + count), pl.ds(base, count)
            branch = sum_two[f, part] + fresh[here, :channels]
            if f == 0:
                sum_two[1, part] += fresh[here, channels:]
            inputs = x_pad[f, 2 + low : 2 + low + size, EDGE:].astype(jnp.float32)
            out[f, low : low + size] = (inputs + branch.reshape(size, cols, channels)).astype(out.dtype)
            at += count

    def stage(f, ones, twos):
        firsts = [multiply_one(f, groups) for groups in ones]
        for groups, fresh in zip(ones, firsts):
            finish_one(f, groups, fresh)
        seconds = [multiply_two(f, groups) for groups in twos]
        for groups, fresh in zip(twos, seconds):
            finish_two(f, groups, fresh)

    def send_tile(f, groups):
        @pl.when(more)
        def _():
            for low, size in groups:
                tile_copy(f, low, size).start()

    borders = [(0, edge), (rows - edge, edge)]
    middle = [(edge, rows - 2 * edge)]

    @pl.when(first)
    def _():
        received(begin[0], MID)
        put_all(taps_one, 3 * pitch, act(0, 3, rows + 2), 0, (rows - 1) * pitch)
        stage(0, [[(3, rows - 4)]], [middle])
        if segments > 1:
            pl.semaphore_wait(ready_sem, plane)
        send_tile(0, middle)
        for stream in held[:1] + begin[:1]:
            received(stream, OUTER)
        put_all(taps_one, 0, act(0, 0, 5), 0, brim)
        put_all(taps_one, rows * pitch + EDGE, act(0, rows, rows + 5), EDGE, 5 * pitch - EDGE)
        held_edge_one()
        ends = [(0, 3), (rows - 1, 3)]
        fresh = multiply_one(0, ends)
        received(held[1], OUTER)
        held_edge_two()
        finish_one(0, ends, fresh, again=True)
        finish_two(0, borders, multiply_two(0, borders))
        start(onward[0], even & more, (-1,))
        start(onward[0], ~even & more, (1,))
        start(onward[0], even & more, (1,))
        start(onward[0], ~even & more, (-1,))
        send_tile(0, borders)

    @pl.when(later)
    def _():
        received(held[0], OUTER)
        held_edge_one()
        received(held[1], OUTER)
        held_edge_two()
        received(onward[0], OUTER)
        received(onward[0], MID, None, True)

    @pl.when(later & more)
    def _():
        act_split(0, rows // 2 + 2)
        tops, lows, mids = [(0, edge + 2)], [(rows - edge, edge + 2)], [(edge + 2, rows - 2 * edge - 2)]
        top, low, mid = (multiply_one(0, groups) for groups in (tops, lows, mids))
        finish_one(0, tops, top)
        top = multiply_two(0, borders[:1])
        finish_one(0, lows, low)
        finish_one(0, mids, mid)
        finish_two(0, borders[:1], top)
        start(onward[0], True, (-1,))
        send_tile(0, borders[:1])
        low, mid = multiply_two(0, borders[1:]), multiply_two(0, middle)
        finish_two(0, borders[1:], low)
        start(onward[0], True, (1,))
        send_tile(0, borders[1:])
        finish_two(0, middle, mid)
        send_tile(0, middle)

    half = rows // 2
    third = (rows + 2) // 6 * 2
    ones = [[(0, third)], [(third, third)], [(2 * third, rows + 2 - 2 * third)]]
    twos = [[(0, third - 2)], [(third - 2, third)], [(2 * third - 2, rows + 2 - 2 * third)]]
    halves = ones, twos

    @pl.when(later & ~more)
    def _():
        act_split(0, half + 3)
        stage(0, *halves)

    start(onward[0], more, (0,))

    for f in range(1, total):
        for group in (MID, OUTER):
            received(begin[f], group, first)
            received(onward[f], group, later, group == MID)
        act_split(f, half + 3)
        stage(f, *halves)
        sent(onward[f - 1], later & more, True, (OUTER,))
        start(onward[f], more, (-1, 1))
        send_tile(f, borders + middle)
        start(onward[f], more, (0,))

    for allowed, share in ((first, 4 + total), (later, 4)):
        settle(
            send_sem.at[0, MID], lambda up, side: cut(one_pad, rows, STRIP * side * share // 2),
            (up_options, side_options), allowed,
        )
        height = 3 if share == 4 else 3 + total
        settle(
            send_sem.at[0, OUTER], lambda up, side: cut(one_pad, height * up, cols + STRIP * side),
            (up_options, side_options), allowed,
        )
    for f in range(total):
        sent(onward[f], first & more, True)
        sent(onward[f], later & more, True, (MID,) if f + 1 < total else (MID, OUTER))


def solution(mesh):
    counts = tuple(mesh.shape[name] for name in ("segment", "row", "col"))

    def on_device(frames, caches, weights, biases, gains):
        total, rows, cols, channels = frames.shape
        pitch = cols + EDGE
        whole = -(-((rows + 2) * pitch + EDGE) // 16) * 16
        bf16, f32 = jnp.bfloat16, jnp.float32
        vmem = pl.BlockSpec(memory_space=pltpu.VMEM)
        taps = weights.reshape(2, TAPS, TAPS * TAPS * channels, channels)
        result = pl.pallas_call(
            functools.partial(kernel, counts),
            out_shape=pltpu.VMEM(frames.shape, bf16),
            in_specs=[pl.BlockSpec(memory_space=pl.ANY)] * 5,
            out_specs=vmem,
            scratch_shapes=[
                pltpu.VMEM(taps.shape, bf16),
                pltpu.VMEM(biases.shape[1:], f32),
                pltpu.VMEM(gains.shape[1:], f32),
                pltpu.VMEM((total, rows + 5, pitch, channels), bf16),
                pltpu.VMEM((2, rows + 5, pitch, channels), bf16),
                pltpu.VMEM((2, rows + 3, pitch, channels), bf16),
                pltpu.VMEM(((rows + 5) * pitch, TAPS * channels), bf16),
                pltpu.VMEM(((rows + 2) * cols, TAPS * channels), bf16),
                pltpu.VMEM((2, (rows + 5) * pitch, TAPS * channels), bf16),
                pltpu.VMEM((2, (rows + 2) * cols, TAPS * channels), bf16),
                pltpu.VMEM((total, whole, channels), f32),
                pltpu.VMEM((total, rows * cols, channels), f32),
                pltpu.VMEM((whole, channels), f32),
                pltpu.SemaphoreType.DMA((1 + total, 2)),
                pltpu.SemaphoreType.DMA((2 + total, 2)),
                pltpu.SemaphoreType.DMA((4,)),
                pltpu.SemaphoreType.REGULAR,
            ],
            compiler_params=pltpu.CompilerParams(collective_id=0, has_side_effects=True),
        )(frames, caches[0], taps, biases[0], gains[0])
        return result[None]

    in_specs = (
        P(None, "row", "col", None),
        P("segment", None, None, "row", "col", None),
        P("segment", None, None, None, None, None, None),
        P("segment", None, None),
        P("segment", None, None),
    )
    out_specs = P("segment", None, "row", "col", None)
    return jax.shard_map(
        on_device, mesh=mesh, in_specs=in_specs, out_specs=out_specs, check_vma=False
    )
```

```python
import functools

import jax
import jax.numpy as jnp
from jax import lax
from jax.experimental import pallas as pl
from jax.experimental.pallas import tpu as pltpu
from jax.sharding import PartitionSpec as P

EDGE = 8
STRIP = 2
TAPS = 3
AROUND = [(dr, dc) for dr in (-1, 1, 0) for dc in (0, -1, 1) if (dr, dc) != (0, 0)]
MID, OUTER = 0, 1


def neighbours(count):
    return {1: (0,), 2: (1,)}.get(count, (1, 2))


def norm_act(values, gain_row):
    scale = lax.rsqrt(jnp.mean(values * values, axis=-1, keepdims=True) + 1e-06)
    half = 0.5 * (values * scale * gain_row)
    return half * jnp.tanh(half) + half


def shifted(values):
    size = values.shape[0]
    return pltpu.roll(values, 1, 0), values, pltpu.roll(values, size - 1, 0)


def kernel(
    counts,
    frames, caches, weights_in, biases_in, gains_in,
    out,
    weights, biases, gains, x_pad, one_pad, two_pad, taps_one, taps_two,
    held_taps_one, held_taps_two, sum_one, sum_two, inside,
    send_sem, recv_sem, local_sem, ready_sem,
):
    segments, tile_rows_n, tile_cols_n = counts
    seg, row, col = (lax.axis_index(name) for name in ("segment", "row", "col"))
    total, rows, cols, channels = frames.shape
    pitch = cols + EDGE
    first = seg == 0
    later = seg > 0
    more = seg < segments - 1

    def exists(dr, dc):
        r, c = row + dr, col + dc
        return (r >= 0) & (r < tile_rows_n) & (c >= 0) & (c < tile_cols_n)

    def device(dz, dr, dc):
        return {"segment": seg + dz, "row": row + dr, "col": col + dc}

    def number(flag):
        return flag.astype(jnp.int32)

    ups = number(row > 0) + number(row < tile_rows_n - 1)
    sides = number(col > 0) + number(col < tile_cols_n - 1)

    def local(source, target, which):
        return pltpu.make_async_copy(source, target, local_sem.at[which])

    def source_rows(dr, base, halo):
        if dr == 0:
            return pl.ds(base, rows)
        return pl.ds(base if dr < 0 else base + rows - halo, halo)

    def source_cols(dc, base):
        if dc == 0:
            return pl.ds(base, cols)
        return pl.ds(base if dc < 0 else base + cols - STRIP, STRIP)

    def target_rows(dr, dc, halo):
        skip = 1 if dc < 0 else 0
        if dr == 0:
            return pl.ds(halo + skip, rows)
        return pl.ds((halo + rows if dr < 0 else 0) + skip, halo)

    def target_cols(dc):
        if dc == 0:
            return pl.ds(EDGE, cols)
        return pl.ds(0, STRIP) if dc < 0 else pl.ds(EDGE - STRIP, STRIP)

    def remote(source, target, halo, send, recv, dz, dr, dc):
        top, left = (0, 0) if dz else (halo, EDGE)
        lead = (slice(None),) * (len(source.shape) - 3)
        group = OUTER if dr else MID
        return pltpu.make_async_remote_copy(
            src_ref=source.at[lead + (source_rows(dr, top, halo), source_cols(dc, left))],
            dst_ref=target.at[lead + (target_rows(dr, dc, halo), target_cols(dc))],
            send_sem=send_sem.at[send, group],
            recv_sem=recv_sem.at[recv, group],
            device_id=device(dz, dr, dc),
            device_id_type=pl.DeviceIdType.MESH,
        )

    held = [(one_pad, one_pad, 2, 0, 0, 0), (two_pad, two_pad, 1, 0, 1, 0)]
    begin = [(x_pad.at[f], x_pad.at[f], 2, 0, 2 + f, 0) for f in range(total)]
    onward = [(out.at[f], x_pad.at[f], 2, 1 + f, 2 + f, 1) for f in range(total)]

    def start(stream, allowed, outer):
        for dr, dc in AROUND:
            if dr not in outer:
                continue
            good = exists(dr, dc)
            if allowed is not True:
                good = good & allowed

            @pl.when(good)
            def _():
                remote(*stream, dr, dc).start()

    def settle(sem, view, options, allowed):
        for up in options[0]:
            for side in options[1]:
                shape = view(up, side)
                if shape is None:
                    continue
                good = (ups == up) & (sides == side)
                if allowed is not None:
                    good = good & allowed

                @pl.when(good)
                def _():
                    pltpu.make_async_copy(shape, shape, sem).wait()

    up_options, side_options = neighbours(tile_rows_n), neighbours(tile_cols_n)

    def cut(ref, height, width):
        if height == 0 or width == 0:
            return None
        lead = (slice(None),) * (len(ref.shape) - 3)
        return ref.at[lead + (pl.ds(0, height), pl.ds(0, width))]

    def settle_group(sems, which, stream, group, allowed, centre):
        ref, halo = stream[1], stream[2]
        middle = cols if centre else 0
        if group == MID:
            view = lambda up, side: cut(ref, rows, middle + STRIP * side)
        else:
            view = lambda up, side: cut(ref, halo * up, cols + STRIP * side)
        settle(sems.at[which, group], view, (up_options, side_options), allowed)

    def received(stream, group, allowed=None, centre=False):
        settle_group(recv_sem, stream[4], stream, group, allowed, centre)

    def sent(stream, allowed=None, centre=False, groups=(MID, OUTER)):
        for group in groups:
            settle_group(send_sem, stream[3], stream, group, allowed, centre)

    edge = rows // 4

    def tile_copy(f, low, size):
        return pltpu.make_async_remote_copy(
            src_ref=out.at[f, pl.ds(low, size)],
            dst_ref=x_pad.at[f, pl.ds(2 + low, size), pl.ds(EDGE, cols)],
            send_sem=send_sem.at[1 + f, MID],
            recv_sem=recv_sem.at[2 + f, MID],
            device_id=device(1, 0, 0),
            device_id_type=pl.DeviceIdType.MESH,
        )

    centre_of = lambda pad, halo: pad.at[:, pl.ds(halo, rows), pl.ds(EDGE, cols)]
    own = local(frames, centre_of(x_pad, 2), 0)
    held_copies = [local(caches.at[0], centre_of(one_pad, 2), 1), local(caches.at[1], centre_of(two_pad, 1), 1)]
    parameters = [local(biases_in, biases, 2), local(gains_in, gains, 2), local(weights_in, weights, 3)]
    few = sum_one.at[0, pl.ds(0, biases.shape[0] + gains.shape[0])]

    @pl.when(first)
    def _():
        own.start()

    for copy in held_copies + parameters:
        copy.start()

    for pad, halo in ((x_pad, 2), (one_pad, 2), (two_pad, 1)):
        count, height = pad.shape[0], pad.shape[1]
        pad[:, :, 0:EDGE] = jnp.zeros((count, height, EDGE, channels), pad.dtype)
        pad[:, 0:halo, EDGE:] = jnp.zeros((count, halo, cols, channels), pad.dtype)
        pad[:, halo + rows :, EDGE:] = jnp.zeros((count, height - halo - rows, cols, channels), pad.dtype)

    def signal_all(semaphore, steps):
        for dz in steps:
            for dr, dc in AROUND + [(0, 0)]:
                if (dz, dr, dc) == (0, 0, 0):
                    continue

                @pl.when(exists(dr, dc) & (seg + dz >= 0) & (seg + dz < segments))
                def _():
                    pl.semaphore_signal(
                        semaphore, inc=1, device_id=device(dz, dr, dc),
                        device_id_type=pl.DeviceIdType.MESH,
                    )

    plane = (ups + 1) * (sides + 1)
    barrier = pltpu.get_barrier_semaphore()
    signal_all(barrier, (0, 1))
    pl.semaphore_wait(barrier, plane - 1 + plane * number(later))

    @pl.when(first)
    def _():
        own.wait()

    local(caches, caches, 1).wait()
    even = row % 2 == 0
    for early in ([(held[0], True), (begin[0], first)], [(held[1], True)]):
        for stream, allowed in early:
            start(stream, even & allowed, (-1,))
            start(stream, ~even & allowed, (1,))
        for stream, allowed in early:
            start(stream, allowed, (0,))
        for stream, allowed in early:
            start(stream, even & allowed, (1,))
            start(stream, ~even & allowed, (-1,))
    for f in range(1, total):
        start(begin[f], first, (-1, 1, 0))
    signal_all(ready_sem, (-1,))

    cell = lax.broadcasted_iota(jnp.int32, inside.shape, 0)
    place = cell % pitch
    wrapped = place < EDGE // 2
    cell_row = row * rows + cell // pitch - 1 - number(wrapped)
    cell_col = col * cols + place - EDGE + jnp.where(wrapped, EDGE + cols, 0)
    inside[...] = jnp.where(
        (cell_row >= 0) & (cell_row < rows * tile_rows_n)
        & (cell_col >= 0) & (cell_col < cols * tile_cols_n), 1.0, 0.0,
    )

    def kernel_of(which, *times):
        return jnp.concatenate([weights[which, t] for t in times], axis=1)

    def patches(store, step, parts):
        return jnp.concatenate(
            [
                jnp.concatenate([store[pl.ds(low + dh * step, size), :] for low, size in parts], axis=0)
                for dh in range(TAPS)
            ],
            axis=1,
        )

    def product(store, step, parts, matrix):
        return jnp.dot(patches(store, step, parts), matrix, preferred_element_type=jnp.float32)

    def flat(pad, index, low, high):
        values = pad[index, low:high].astype(jnp.float32)
        return values.reshape((high - low) * pitch, channels)

    def put_all(store, low, values, skip, size):
        for tap, part in enumerate(shifted(values)):
            store[pl.ds(low, size), tap * channels : (tap + 1) * channels] = (
                part[skip : skip + size].astype(jnp.bfloat16)
            )

    def put_tile(store, low, values, height):
        for tap, part in enumerate(shifted(values)):
            part = part[: height * pitch].reshape(height, pitch, channels)[:, EDGE:]
            store[pl.ds(low * cols, height * cols), tap * channels : (tap + 1) * channels] = (
                part.reshape(height * cols, channels).astype(jnp.bfloat16)
            )

    def add_cached(which, store, sums, step, parts):
        bias = biases[which : which + 1]
        older = product(store.at[0], step, parts, kernel_of(which, 0))
        newer = product(store.at[1], step, parts, kernel_of(which, 1, 0))
        at = 0
        for low, size in parts:
            here = slice(at, at + size)
            sums[0, pl.ds(low, size)] = older[here] + newer[here, :channels] + bias
            sums[1, pl.ds(low, size)] = newer[here, channels:] + bias
            at += size

    local(few, few, 2).wait()
    parameters[-1].wait()

    whole = sum_one.shape[1]
    brim = -(-(3 * pitch + EDGE) // 16) * 16
    rest = (rows - 1) * pitch
    received(held[0], MID)
    for frame in range(2):
        put_all(
            held_taps_one.at[frame], 3 * pitch, flat(one_pad, frame, 3, rows + 2), 0, (rows - 1) * pitch
        )
    low = 3 * pitch
    add_cached(0, held_taps_one, sum_one, pitch, [(low, (rows - 1) * pitch + EDGE - low)])
    received(held[1], MID)
    for frame in range(2):
        put_tile(held_taps_two.at[frame], 2, flat(two_pad, frame, 2, rows + 1), rows - 2)
    add_cached(1, held_taps_two, sum_two, cols, [(2 * cols, (rows - 4) * cols)])

    @pl.when(more & later)
    def _():
        pl.semaphore_wait(ready_sem, plane)

    def held_edge_one():
        for frame in range(2):
            put_all(held_taps_one.at[frame], 0, flat(one_pad, frame, 0, 5), 0, brim)
            values = flat(one_pad, frame, rows, rows + 5)
            put_all(held_taps_one.at[frame], rows * pitch + EDGE, values, EDGE, 5 * pitch - EDGE)
        add_cached(0, held_taps_one, sum_one, pitch, [(0, brim), (rest, whole - rest)])

    def held_edge_two():
        for frame in range(2):
            put_tile(held_taps_two.at[frame], 0, flat(two_pad, frame, 0, 3), 2)
            put_tile(held_taps_two.at[frame], rows, flat(two_pad, frame, rows, rows + 3), 2)
        add_cached(1, held_taps_two, sum_two, cols, [(0, 2 * cols), ((rows - 2) * cols, 2 * cols)])

    def matrix(which, f):
        return kernel_of(which, *((2, 1) if f == 0 else (2,)))

    def act(f, low, high):
        return norm_act(flat(x_pad, f, low, high), gains[0:1])

    def act_split(f, at):
        put_all(taps_one, 0, act(f, 0, at + 1), 0, at * pitch)
        put_all(taps_one, at * pitch, act(f, at - 1, rows + 5), pitch, (rows + 5 - at) * pitch)

    def spans_one(groups):
        return [
            (low * pitch, whole - low * pitch if low + height == rows + 2 else height * pitch + EDGE)
            for low, height in groups
        ]

    def spans_two(groups):
        return [(low * cols, size * cols) for low, size in groups]

    def multiply_one(f, groups):
        return product(taps_one, pitch, spans_one(groups), matrix(0, f))

    def multiply_two(f, groups):
        return product(taps_two, cols, spans_two(groups), matrix(1, f))

    def finish_one(f, groups, fresh, again=False):
        at = 0
        for (low, height), (base, size) in zip(groups, spans_one(groups)):
            part = pl.ds(base, size)
            hidden = sum_one[f, part] + fresh[at : at + size, :channels]
            if f == 0:
                keep = size if low + height == rows + 2 or again else height * pitch
                sum_one[1, pl.ds(base, keep)] += fresh[at : at + keep, channels:]
            put_tile(taps_two, low, norm_act(hidden, gains[1:2]) * inside[part], height)
            at += size

    def finish_two(f, groups, fresh):
        at = 0
        for (low, size), (base, count) in zip(groups, spans_two(groups)):
            here, part = slice(at, at + count), pl.ds(base, count)
            branch = sum_two[f, part] + fresh[here, :channels]
            if f == 0:
                sum_two[1, part] += fresh[here, channels:]
            inputs = x_pad[f, 2 + low : 2 + low + size, EDGE:].astype(jnp.float32)
            out[f, low : low + size] = (inputs + branch.reshape(size, cols, channels)).astype(out.dtype)
            at += count

    def stage(f, ones, twos):
        firsts = [multiply_one(f, groups) for groups in ones]
        for groups, fresh in zip(ones, firsts):
            finish_one(f, groups, fresh)
        seconds = [multiply_two(f, groups) for groups in twos]
        for groups, fresh in zip(twos, seconds):
            finish_two(f, groups, fresh)

    def send_tile(f, groups):
        @pl.when(more)
        def _():
            for low, size in groups:
                tile_copy(f, low, size).start()

    borders = [(0, edge), (rows - edge, edge)]
    middle = [(edge, rows - 2 * edge)]

    @pl.when(first)
    def _():
        received(begin[0], MID)
        put_all(taps_one, 3 * pitch, act(0, 3, rows + 2), 0, (rows - 1) * pitch)
        stage(0, [[(3, rows - 4)]], [middle])
        if segments > 1:
            pl.semaphore_wait(ready_sem, plane)
        send_tile(0, middle)
        for stream in held[:1] + begin[:1]:
            received(stream, OUTER)
        put_all(taps_one, 0, act(0, 0, 5), 0, brim)
        put_all(taps_one, rows * pitch + EDGE, act(0, rows, rows + 5), EDGE, 5 * pitch - EDGE)
        held_edge_one()
        ends = [(0, 3), (rows - 1, 3)]
        fresh = multiply_one(0, ends)
        received(held[1], OUTER)
        held_edge_two()
        finish_one(0, ends, fresh, again=True)
        finish_two(0, borders, multiply_two(0, borders))
        start(onward[0], even & more, (-1,))
        start(onward[0], ~even & more, (1,))
        start(onward[0], even & more, (1,))
        start(onward[0], ~even & more, (-1,))
        send_tile(0, borders)

    @pl.when(later)
    def _():
        received(held[0], OUTER)
        held_edge_one()
        received(held[1], OUTER)
        held_edge_two()
        received(onward[0], OUTER)
        received(onward[0], MID, None, True)

    @pl.when(later & more)
    def _():
        act_split(0, rows // 2 + 2)
        tops, lows, mids = [(0, edge + 2)], [(rows - edge, edge + 2)], [(edge + 2, rows - 2 * edge - 2)]
        top, low, mid = (multiply_one(0, groups) for groups in (tops, lows, mids))
        finish_one(0, tops, top)
        top = multiply_two(0, borders[:1])
        finish_one(0, lows, low)
        finish_one(0, mids, mid)
        finish_two(0, borders[:1], top)
        start(onward[0], True, (-1,))
        send_tile(0, borders[:1])
        finish_two(0, borders[1:], multiply_two(0, borders[1:]))
        start(onward[0], True, (1,))
        send_tile(0, borders[1:])
        finish_two(0, middle, multiply_two(0, middle))
        send_tile(0, middle)

    half = rows // 2
    third = (rows + 2) // 6 * 2
    ones = [[(0, third)], [(third, third)], [(2 * third, rows + 2 - 2 * third)]]
    twos = [[(0, third - 2)], [(third - 2, third)], [(2 * third - 2, rows + 2 - 2 * third)]]
    halves = ones, twos

    @pl.when(later & ~more)
    def _():
        act_split(0, half + 3)
        stage(0, *halves)

    start(onward[0], more, (0,))

    for f in range(1, total):
        for group in (MID, OUTER):
            received(begin[f], group, first)
            received(onward[f], group, later, group == MID)
        act_split(f, half + 3)
        stage(f, *halves)
        sent(onward[f - 1], later & more, True, (OUTER,))
        start(onward[f], more, (-1, 1))
        send_tile(f, borders + middle)
        start(onward[f], more, (0,))

    for allowed, share in ((first, 4 + total), (later, 4)):
        settle(
            send_sem.at[0, MID], lambda up, side: cut(one_pad, rows, STRIP * side * share // 2),
            (up_options, side_options), allowed,
        )
        height = 3 if share == 4 else 3 + total
        settle(
            send_sem.at[0, OUTER], lambda up, side: cut(one_pad, height * up, cols + STRIP * side),
            (up_options, side_options), allowed,
        )
    for f in range(total):
        sent(onward[f], first & more, True)
        sent(onward[f], later & more, True, (MID,) if f + 1 < total else (MID, OUTER))


def solution(mesh):
    counts = tuple(mesh.shape[name] for name in ("segment", "row", "col"))

    def on_device(frames, caches, weights, biases, gains):
        total, rows, cols, channels = frames.shape
        pitch = cols + EDGE
        whole = -(-((rows + 2) * pitch + EDGE) // 16) * 16
        bf16, f32 = jnp.bfloat16, jnp.float32
        vmem = pl.BlockSpec(memory_space=pltpu.VMEM)
        taps = weights.reshape(2, TAPS, TAPS * TAPS * channels, channels)
        result = pl.pallas_call(
            functools.partial(kernel, counts),
            out_shape=pltpu.VMEM(frames.shape, bf16),
            in_specs=[pl.BlockSpec(memory_space=pl.ANY)] * 5,
            out_specs=vmem,
            scratch_shapes=[
                pltpu.VMEM(taps.shape, bf16),
                pltpu.VMEM(biases.shape[1:], f32),
                pltpu.VMEM(gains.shape[1:], f32),
                pltpu.VMEM((total, rows + 5, pitch, channels), bf16),
                pltpu.VMEM((2, rows + 5, pitch, channels), bf16),
                pltpu.VMEM((2, rows + 3, pitch, channels), bf16),
                pltpu.VMEM(((rows + 5) * pitch, TAPS * channels), bf16),
                pltpu.VMEM(((rows + 2) * cols, TAPS * channels), bf16),
                pltpu.VMEM((2, (rows + 5) * pitch, TAPS * channels), bf16),
                pltpu.VMEM((2, (rows + 2) * cols, TAPS * channels), bf16),
                pltpu.VMEM((total, whole, channels), f32),
                pltpu.VMEM((total, rows * cols, channels), f32),
                pltpu.VMEM((whole, channels), f32),
                pltpu.SemaphoreType.DMA((1 + total, 2)),
                pltpu.SemaphoreType.DMA((2 + total, 2)),
                pltpu.SemaphoreType.DMA((4,)),
                pltpu.SemaphoreType.REGULAR,
            ],
            compiler_params=pltpu.CompilerParams(collective_id=0, has_side_effects=True),
        )(frames, caches[0], taps, biases[0], gains[0])
        return result[None]

    in_specs = (
        P(None, "row", "col", None),
        P("segment", None, None, "row", "col", None),
        P("segment", None, None, None, None, None, None),
        P("segment", None, None),
        P("segment", None, None),
    )
    out_specs = P("segment", None, "row", "col", None)
    return jax.shard_map(
        on_device, mesh=mesh, in_specs=in_specs, out_specs=out_specs, check_vma=False
    )
```
